8 devices in a mesh: dp: 2 (over z, y), tp: 4 (over x, core).
Axes of the slice: x: 2, y: 2, z: 1, core: 2. Of those that a mesh axis runs over, the one named last changes fastest.
Arguments:
- hidden: bfloat16 [8, 1024, 2560], P('dp', 'tp'), parts along dimension 0
- ln1_gain: float32 [2560], replicated
- ln1_bias: float32 [2560], replicated
- w_qkv: bfloat16 [2560, 3, 32, 80], P(None, None, 'tp')
- b_qkv: bfloat16 [3, 32, 80], P(None, 'tp')
- w_out: bfloat16 [32, 80, 2560], P('tp')
- b_out: bfloat16 [2560], replicated
- ln2_gain: float32 [2560], replicated
- ln2_bias: float32 [2560], replicated
- w_up: bfloat16 [2560, 10240], P(None, 'tp')
- b_up: bfloat16 [10240], P('tp')
- w_down: bfloat16 [10240, 2560], P('tp')
- b_down: bfloat16 [2560], replicated
Outputs:
- output: bfloat16 [8, 1024, 2560], P('dp', 'tp'), parts along dimension 0
There are 2 independent parts. The reference program is written for one: setup_inputs(seed, part) draws one part's arguments, and reference() takes and returns one part's arrays. A program takes and returns all parts, laid end to end along the dimension named above; an argument that names none is the same for every part.
All inputs are finite; a program needn't handle non-finite values.
Results may differ from the reference program's by a relative error of at most 0.0106374.
Values are sent between devices in bfloat16 or wider.
A program may use at most 1 GiB of HBM per device.

```python
import math
import jax
import jax.numpy as jnp
from jax import lax

N_BATCH = 4
SEQ_LEN = 1024
D_MODEL = 2560
N_HEADS = 32

HEAD_DIM = D_MODEL // N_HEADS
FF_DIM = 4 * D_MODEL
LN_EPS = 1e-5


def layer_norm(inputs, gain_vec, shift_vec):
    as_f32 = inputs.astype(jnp.float32)
    row_mean = jnp.mean(as_f32, axis=-1, keepdims=True)
    centered = as_f32 - row_mean
    variance = jnp.mean(centered * centered, axis=-1, keepdims=True)
    return (centered * lax.rsqrt(variance + LN_EPS) * gain_vec + shift_vec).astype(jnp.bfloat16)


def setup_inputs(seed: int = 0, part: int = 0) -> dict:
    root_key = jax.random.key(seed)
    sub_keys = jax.random.split(root_key, 13)
    qk_gain = (0.5 * math.log(SEQ_LEN)) ** 0.25
    col_gain = jnp.array([qk_gain, qk_gain, 1.0], jnp.float32).reshape(1, 3, 1, 1)
    hidden = jax.random.normal(jax.random.fold_in(sub_keys[0], part), (N_BATCH, SEQ_LEN, D_MODEL), jnp.float32)
    w_qkv = jax.random.normal(sub_keys[3], (D_MODEL, 3, N_HEADS, HEAD_DIM), jnp.float32) * col_gain * D_MODEL ** -0.5
    return {
        "hidden": hidden.astype(jnp.bfloat16),
        "ln1_gain": 1.0 + 0.3 * jax.random.normal(sub_keys[1], (D_MODEL,), jnp.float32),
        "ln1_bias": 0.3 * jax.random.normal(sub_keys[2], (D_MODEL,), jnp.float32),
        "w_qkv": w_qkv.astype(jnp.bfloat16),
        "b_qkv": (0.5 * jax.random.normal(sub_keys[4], (3, N_HEADS, HEAD_DIM), jnp.float32)).astype(jnp.bfloat16),
        "w_out": (jax.random.normal(sub_keys[5], (N_HEADS, HEAD_DIM, D_MODEL), jnp.float32) * D_MODEL ** -0.5).astype(jnp.bfloat16),
        "b_out": (0.3 * jax.random.normal(sub_keys[6], (D_MODEL,), jnp.float32)).astype(jnp.bfloat16),
        "ln2_gain": 1.0 + 0.3 * jax.random.normal(sub_keys[7], (D_MODEL,), jnp.float32),
        "ln2_bias": 0.3 * jax.random.normal(sub_keys[8], (D_MODEL,), jnp.float32),
        "w_up": (jax.random.normal(sub_keys[9], (D_MODEL, FF_DIM), jnp.float32) * D_MODEL ** -0.5).astype(jnp.bfloat16),
        "b_up": (0.5 * jax.random.normal(sub_keys[10], (FF_DIM,), jnp.float32)).astype(jnp.bfloat16),
        "w_down": (jax.random.normal(sub_keys[11], (FF_DIM, D_MODEL), jnp.float32) * FF_DIM ** -0.5).astype(jnp.bfloat16),
        "b_down": (0.3 * jax.random.normal(sub_keys[12], (D_MODEL,), jnp.float32)).astype(jnp.bfloat16),
    }


def reference(hidden, ln1_gain, ln1_bias, w_qkv, b_qkv, w_out, b_out, ln2_gain, ln2_bias, w_up, b_up, w_down, b_down):
    normed = layer_norm(hidden, ln1_gain, ln1_bias).reshape(N_BATCH * SEQ_LEN, D_MODEL)
    qkv_acc = jnp.dot(normed, w_qkv.reshape(D_MODEL, 3 * D_MODEL), preferred_element_type=jnp.float32)
    qkv_all = (qkv_acc + b_qkv.reshape(3 * D_MODEL).astype(jnp.float32)).astype(jnp.bfloat16)
    head_major = jnp.transpose(qkv_all.reshape(N_BATCH, SEQ_LEN, 3, N_HEADS, HEAD_DIM), (2, 3, 0, 1, 4))
    positions = jnp.arange(SEQ_LEN)
    causal = positions[:, None] >= positions[None, :]

    def one_head(operands):
        queries, keys_all, values = operands
        logits = jnp.einsum("bqd,bkd->bqk", queries.astype(jnp.float32), keys_all.astype(jnp.float32)) * HEAD_DIM ** -0.5
        logits = jnp.where(causal, logits, -1e30)
        row_max = jnp.max(logits, axis=-1, keepdims=True)
        exp_vals = jnp.exp(logits - row_max)
        weights_bf = (exp_vals / jnp.sum(exp_vals, axis=-1, keepdims=True)).astype(jnp.bfloat16)
        return jnp.einsum("bqk,bkd->bqd", weights_bf.astype(jnp.float32), values.astype(jnp.float32)).astype(jnp.bfloat16)

    context = lax.map(one_head, (head_major[0], head_major[1], head_major[2]))
    attn_sum = jnp.einsum("hbsd,hde->bse", context.astype(jnp.float32), w_out.astype(jnp.float32))
    resid_mid = (hidden.astype(jnp.float32) + (attn_sum + b_out.astype(jnp.float32))).astype(jnp.bfloat16)
    normed_mid = layer_norm(resid_mid, ln2_gain, ln2_bias).reshape(N_BATCH * SEQ_LEN, D_MODEL)
    up_proj = jnp.dot(normed_mid, w_up, preferred_element_type=jnp.float32) + b_up.astype(jnp.float32)
    gelu_out = jax.nn.gelu(up_proj, approximate=True).astype(jnp.bfloat16)
    down_sum = jnp.dot(gelu_out, w_down, preferred_element_type=jnp.float32) + b_down.astype(jnp.float32)
    return (resid_mid.astype(jnp.float32) + down_sum.reshape(N_BATCH, SEQ_LEN, D_MODEL)).astype(jnp.bfloat16)
```

```python
import functools

import jax
import jax.numpy as jnp
from jax import lax
from jax.experimental import pallas as pl
from jax.experimental.pallas import tpu as pltpu
from jax.sharding import PartitionSpec as P


LN_EPS = 1e-5
BF16 = jnp.bfloat16
F32 = jnp.float32


CHUNK = 32


def normalize(x, gain, shift):
    as_f32 = x.astype(F32)
    row_mean = jnp.mean(as_f32, axis=-1, keepdims=True)
    centered = as_f32 - row_mean
    variance = jnp.mean(centered * centered, axis=-1, keepdims=True)
    return (centered * lax.rsqrt(variance + LN_EPS) * gain + shift).astype(BF16)


def params(mib):
    return pltpu.CompilerParams(dimension_semantics=("arbitrary",), vmem_limit_bytes=mib << 20)


def qkv_kernel(n_x, n_w, steps, *refs):
    x_refs, (gain_ref, shift_ref) = refs[:n_x], refs[n_x:n_x + 2]
    w_refs, b_refs = refs[n_x + 2:n_x + 2 + n_w], refs[n_x + 2 + n_w:n_x + 2 + 2 * n_w]
    o_refs, normed = refs[n_x + 2 + 2 * n_w:-1], refs[-1]
    block = x_refs[0].shape[-2]
    step = pl.program_id(0)

    @pl.when(step == 0)
    def _():
        for p in range(n_x):
            @pl.loop(0, block // CHUNK)
            def _(r):
                rows = pl.ds(pl.multiple_of(r * CHUNK, CHUNK), CHUNK)
                out_rows = pl.ds(pl.multiple_of(p * block + r * CHUNK, CHUNK), CHUNK)
                normed[out_rows, :] = normalize(x_refs[p][0, rows, :], gain_ref[...], shift_ref[...])

    for t in range(n_w):
        @pl.when((step >= t * steps) & (step < (t + 1) * steps))
        def _():
            acc = lax.dot_general(normed[...], w_refs[t][...], (((1,), (1,)), ((), ())), preferred_element_type=F32)
            out = (acc + b_refs[t][...].astype(F32)).astype(BF16)
            o_refs[t][...] = out.reshape(o_refs[t].shape)


def qkv_projection(xs, gain, shift, ws, bs):
    arrays = [a for a, _ in xs]
    n_x, n_w = len(xs), len(ws)
    _, block, d_model = arrays[0].shape
    n_cols = ws[0].shape[0]
    tile = 640
    steps = n_cols // tile
    place = lambda t: (lambda i: jnp.clip(i - t * steps, 0, steps - 1))
    x_specs = [pl.BlockSpec((1, block, d_model), lambda i, k=k: (k, 0, 0)) for _, k in xs]
    vec = pl.BlockSpec((1, d_model), lambda i: (0, 0))
    w_specs = [pl.BlockSpec((tile, d_model), lambda i, f=place(t): (f(i), 0)) for t in range(n_w)]
    b_specs = [pl.BlockSpec((1, tile), lambda i, f=place(t): (0, f(i))) for t in range(n_w)]
    o_specs = [pl.BlockSpec((n_x, block, tile), lambda i, f=place(t): (0, 0, f(i))) for t in range(n_w)]
    return pl.pallas_call(
        functools.partial(qkv_kernel, n_x, n_w, steps),
        out_shape=[jax.ShapeDtypeStruct((n_x, block, n_cols), BF16)] * n_w,
        grid=(n_w * steps,),
        in_specs=x_specs + [vec, vec] + w_specs + b_specs,
        out_specs=o_specs,
        scratch_shapes=[pltpu.VMEM((n_x * block, d_model), BF16)],
        compiler_params=params(56),
        cost_estimate=pl.CostEstimate(
            flops=2 * n_x * block * d_model * n_cols * n_w,
            bytes_accessed=2 * (n_x * block * (d_model + n_w * n_cols) + n_w * n_cols * d_model),
            transcendentals=0),
    )(*arrays, gain, shift, *ws, *bs)


def out_kernel(x0_ref, x1_ref, b_ref, gain_ref, shift_ref, c0, c1, c2, c3, w0, w1, w2, w3, *refs):
    o_refs, (ctx, weight, resid) = refs[:-3], refs[-3:]
    normed_ref = o_refs[-1]
    step = pl.program_id(0)
    n_half, block, width = c0.shape
    tile = w0.shape[1]

    @pl.when(step == 0)
    def _():
        for j, c in enumerate((c0, c1, c2, c3)):
            for p in range(n_half):
                ctx[p * block:(p + 1) * block, j * width:(j + 1) * width] = c[p]

    for j, w in enumerate((w0, w1, w2, w3)):
        weight[j * width:(j + 1) * width, :] = w[...]
    acc = jnp.dot(ctx[...], weight[...], preferred_element_type=F32) + b_ref[...].astype(F32)
    cols = pl.ds(pl.multiple_of(step * tile, tile), tile)
    for p, x in enumerate((x0_ref, x1_ref)):
        rows = slice(p * block, (p + 1) * block)
        resid[rows, cols] = (x[0, :, cols].astype(F32) + acc[rows]).astype(BF16)

    @pl.when(step == pl.num_programs(0) - 1)
    def _():
        @pl.loop(0, n_half * block // CHUNK)
        def _(r):
            rows = pl.ds(pl.multiple_of(r * CHUNK, CHUNK), CHUNK)
            normed_ref[rows, :] = normalize(resid[rows, :], gain_ref[...], shift_ref[...])
            if len(o_refs) > 1:
                o_refs[0][rows, :] = resid[rows, :]


def out_projection(xs, bias, gain, shift, ctx, halves, ws, keep):
    arrays = [a for a, _ in xs]
    _, block, d_model = arrays[0].shape
    width = ws[0].shape[0]
    tile = 512
    rows = 2 * block
    x_specs = [pl.BlockSpec((1, block, d_model), lambda i, k=k: (k, 0, 0)) for _, k in xs]
    vec = pl.BlockSpec((1, d_model), lambda i: (0, 0))
    c_specs = [pl.BlockSpec((2, block, width), lambda i, h=h: (h, 0, 0)) for h in halves]
    w_specs = [pl.BlockSpec((width, tile), lambda i: (0, i))] * 4
    n_out = 2 if keep else 1
    out = pl.pallas_call(
        out_kernel,
        out_shape=[jax.ShapeDtypeStruct((rows, d_model), BF16)] * n_out,
        grid=(d_model // tile,),
        in_specs=x_specs + [pl.BlockSpec((1, tile), lambda i: (0, i)), vec, vec] + c_specs + w_specs,
        out_specs=[pl.BlockSpec((rows, d_model), lambda i: (0, 0))] * n_out,
        scratch_shapes=[pltpu.VMEM((rows, 4 * width), BF16), pltpu.VMEM((4 * width, tile), BF16), pltpu.VMEM((rows, d_model), BF16)],
        compiler_params=params(56),
        cost_estimate=pl.CostEstimate(
            flops=2 * rows * d_model * 4 * width,
            bytes_accessed=2 * (rows * (d_model * (1 + n_out) + 4 * width) + 4 * width * d_model),
            transcendentals=0),
    )(*arrays, bias, gain, shift, *ctx, *ws)
    return out if keep else (None, out[0])


def mlp_kernel(n_w, steps, h_ref, *refs):
    up_refs, b_refs, down_refs = refs[:n_w], refs[n_w:2 * n_w], refs[2 * n_w:3 * n_w]
    o_ref, acc = refs[3 * n_w:]
    step = pl.program_id(0)
    for t in range(n_w):
        @pl.when((step >= t * steps) & (step < (t + 1) * steps))
        def _():
            up = jnp.dot(h_ref[...], up_refs[t][...], preferred_element_type=F32) + b_refs[t][...].astype(F32)
            act = jax.nn.gelu(up, approximate=True).astype(BF16)
            part = jnp.dot(act, down_refs[t][...], preferred_element_type=F32)
            if t == 0:
                acc[...] = jnp.where(step == 0, part, acc[...] + part)
            else:
                acc[...] += part

    @pl.when(step == pl.num_programs(0) - 1)
    def _():
        o_ref[...] = acc[...].astype(o_ref.dtype)


def mlp(normed, ups, bs, downs, out_type):
    rows, d_model = normed.shape
    n_w = len(ups)
    n_cols = ups[0].shape[1]
    tile = 512
    steps = n_cols // tile
    place = lambda t: (lambda i: jnp.clip(i - t * steps, 0, steps - 1))
    whole = pl.BlockSpec((rows, d_model), lambda i: (0, 0))
    return pl.pallas_call(
        functools.partial(mlp_kernel, n_w, steps),
        out_shape=jax.ShapeDtypeStruct((rows, d_model), out_type),
        grid=(n_w * steps,),
        in_specs=[whole]
        + [pl.BlockSpec((d_model, tile), lambda i, f=place(t): (0, f(i))) for t in range(n_w)]
        + [pl.BlockSpec((1, tile), lambda i, f=place(t): (0, f(i))) for t in range(n_w)]
        + [pl.BlockSpec((tile, d_model), lambda i, f=place(t): (f(i), 0)) for t in range(n_w)],
        out_specs=whole,
        scratch_shapes=[pltpu.VMEM((rows, d_model), F32)],
        compiler_params=params(60),
        cost_estimate=pl.CostEstimate(
            flops=4 * rows * d_model * n_cols * n_w,
            bytes_accessed=2 * n_w * 2 * n_cols * d_model + 6 * rows * d_model,
            transcendentals=rows * n_cols * n_w),
    )(normed, *ups, *bs, *downs)


def attention_kernel(head_dim, window, me_ref, local_ref, remote_ref, ctx_ref, ordered):
    head = pl.program_id(0)
    me = me_ref[0]
    n_slots, block, width = ctx_ref.shape
    half = n_slots // 2

    @pl.when(head == 0)
    def _():
        for slot in range(n_slots):
            source = local_ref if slot < half else remote_ref
            ordered[me ^ slot] = source[slot % half]

    first = head * head_dim
    start = jnp.minimum((first // 128) * 128, width - window)
    start = pl.multiple_of(start, 128)
    lane = lax.broadcasted_iota(jnp.int32, (block, window), 1) + start
    in_head = (lane >= first) & (lane < first + head_dim)
    scale = head_dim ** -0.5
    rows = lax.broadcasted_iota(jnp.int32, (block, block), 0)
    cols = lax.broadcasted_iota(jnp.int32, (block, block), 1)
    contract_last = (((1,), (1,)), ((), ()))
    for g in range(n_slots):
        q = ordered[g, :, pl.ds(start, window)]
        q = jnp.where(in_head, q, jnp.zeros_like(q))
        diag_k = ordered[g, :, pl.ds(width + start, window)]
        diag = lax.dot_general(q, diag_k, contract_last, preferred_element_type=F32) * scale
        diag = jnp.where(rows >= cols, diag, -1e30)
        row_max = jnp.max(diag, axis=-1, keepdims=True)
        if g:
            k = ordered[0:g, :, pl.ds(width + start, window)].reshape(g * block, window)
            full = lax.dot_general(q, k, contract_last, preferred_element_type=F32) * scale
            row_max = jnp.maximum(row_max, jnp.max(full, axis=-1, keepdims=True))
        diag = jnp.exp(diag - row_max)
        total = jnp.sum(diag, axis=-1, keepdims=True)
        if g:
            full = jnp.exp(full - row_max)
            total = total + jnp.sum(full, axis=-1, keepdims=True)
        inverse = 1.0 / total
        diag_v = ordered[g, :, pl.ds(2 * width + start, window)]
        ctx = jnp.dot((diag * inverse).astype(BF16), diag_v, preferred_element_type=F32)
        if g:
            v = ordered[0:g, :, pl.ds(2 * width + start, window)].reshape(g * block, window)
            ctx = ctx + jnp.dot((full * inverse).astype(BF16), v, preferred_element_type=F32)
        slot = me ^ g
        old = ctx_ref[slot, :, pl.ds(start, window)]
        ctx_ref[slot, :, pl.ds(start, window)] = jnp.where(in_head, ctx.astype(BF16), old)


def attention(me, qkv_local, local_at, qkv_remote, n_heads, head_dim):
    n_half, block, three_width = qkv_remote.shape
    width = three_width // 3
    n_slots = 2 * n_half
    window = 256
    pairs = n_slots * (n_slots + 1) // 2
    whole = lambda *_: (0, 0, 0)
    return pl.pallas_call(
        functools.partial(attention_kernel, head_dim, window),
        out_shape=jax.ShapeDtypeStruct((n_slots, block, width), BF16),
        grid_spec=pltpu.PrefetchScalarGridSpec(
            num_scalar_prefetch=1,
            grid=(n_heads,),
            in_specs=[pl.BlockSpec((n_half, block, three_width), lambda *_: (local_at, 0, 0)), pl.BlockSpec(qkv_remote.shape, whole)],
            out_specs=pl.BlockSpec((n_slots, block, width), whole),
            scratch_shapes=[pltpu.VMEM((n_slots, block, three_width), BF16)],
        ),
        compiler_params=pltpu.CompilerParams(dimension_semantics=("arbitrary",), vmem_limit_bytes=40 << 20),
        cost_estimate=pl.CostEstimate(
            flops=n_heads * pairs * block * block * window * 4,
            bytes_accessed=n_slots * block * width * 8,
            transcendentals=n_heads * pairs * block * block,
        ),
    )(me, qkv_local, qkv_remote)


def finish_kernel(steps, core_ref, part_ref, arrived_ref, resid_ref, b_ref, *refs):
    mine_ref, other_ref = refs[-2:]
    total = part_ref[...] + arrived_ref[...].astype(F32)
    done = (resid_ref[...].astype(F32) + (total + b_ref[...].astype(F32))).astype(BF16)
    step = pl.program_id(0)

    @pl.when(step < steps)
    def _():
        mine_ref[0] = done

    @pl.when(step >= steps)
    def _():
        other_ref[...] = done


def finish(core, part, arrived, resid, bias, s, n_batch, out):
    rows, d_model = part.shape
    block = rows // 2
    tile = 128
    steps = block // tile
    n_mine = n_batch // 2
    spec = pl.BlockSpec((tile, d_model), lambda i, c: (i, 0))
    extra = [] if out is None else [out]
    return pl.pallas_call(
        functools.partial(finish_kernel, steps),
        out_shape=[jax.ShapeDtypeStruct((n_batch, block, d_model), BF16), jax.ShapeDtypeStruct((block, d_model), BF16)],
        grid_spec=pltpu.PrefetchScalarGridSpec(
            num_scalar_prefetch=1,
            grid=(2 * steps,),
            in_specs=[spec, spec, spec, pl.BlockSpec((1, d_model), lambda i, c: (0, 0))] + [pl.BlockSpec(memory_space=pl.ANY)] * len(extra),
            out_specs=[
                pl.BlockSpec((1, tile, d_model), lambda i, c: (c[0] * n_mine + s, jnp.minimum(i, steps - 1), 0)),
                pl.BlockSpec((tile, d_model), lambda i, c: (jnp.maximum(i - steps, 0), 0)),
            ],
        ),
        input_output_aliases={5: 0} if extra else {},
        compiler_params=params(40),
        cost_estimate=pl.CostEstimate(flops=rows * d_model * 4, bytes_accessed=10 * rows * d_model, transcendentals=0),
    )(core, part, arrived, resid, bias, *extra)


def place_kernel(core_ref, block_ref, out_in_ref, out_ref):
    out_ref[0] = block_ref[...]


def place(core, piece, s, out):
    n_batch, block, d_model = out.shape
    n_mine = n_batch // 2
    tile = 128
    return pl.pallas_call(
        place_kernel,
        out_shape=jax.ShapeDtypeStruct(out.shape, BF16),
        grid_spec=pltpu.PrefetchScalarGridSpec(
            num_scalar_prefetch=1,
            grid=(block // tile,),
            in_specs=[pl.BlockSpec((tile, d_model), lambda i, c: (i, 0)), pl.BlockSpec(memory_space=pl.ANY)],
            out_specs=pl.BlockSpec((1, tile, d_model), lambda i, c: ((1 - c[0]) * n_mine + s, i, 0)),
        ),
        input_output_aliases={2: 0},
        compiler_params=params(40),
        cost_estimate=pl.CostEstimate(flops=block * d_model, bytes_accessed=4 * block * d_model, transcendentals=0),
    )(core, piece, out)


def solution(mesh):
    group_size = mesh.shape["tp"]
    n_groups = mesh.shape["dp"]

    def swap(array, mask):
        return lax.ppermute(array, "tp", [(i, i ^ mask) for i in range(group_size)])

    def device_body(hidden, ln1_gain, ln1_bias, w_qkv, b_qkv, w_out, b_out, ln2_gain, ln2_bias, w_up, b_up, w_down, b_down):
        n_batch, _, d_model = hidden.shape
        _, _, n_heads, head_dim = w_qkv.shape
        width = n_heads * head_dim
        me = lax.axis_index("tp")
        core = me % 2
        group = lax.axis_index("dp")
        n_mine = n_batch // 2
        row = lambda v: v.reshape(1, -1)

        mine = lax.dynamic_slice_in_dim(hidden, core * n_mine, n_mine, 0)
        other = lax.dynamic_slice_in_dim(hidden, (1 - core) * n_mine, n_mine, 0)

        slot2 = [swap(mine[s:s + 1], 2) for s in range(n_mine)]
        slot3 = [swap(other[s:s + 1], 3) for s in range(n_mine)]
        slot1 = swap(other, 1)
        x_local = [[(mine, s), (slot1, s)] for s in range(n_mine)]
        x_remote = [[(slot2[s], 0), (slot3[s], 0)] for s in range(n_mine)]

        w_qkv_t = jnp.transpose(w_qkv, (1, 2, 3, 0)).reshape(3 * width, d_model)
        w_qkv_of = [w_qkv_t, swap(w_qkv_t, 1)]
        b_qkv_flat = row(b_qkv)
        b_qkv_of = [b_qkv_flat, swap(b_qkv_flat, 1)]
        w_out_flat = w_out.reshape(width, d_model)
        half_rows = width // n_groups
        near = swap(lax.dynamic_slice_in_dim(w_out_flat, group * half_rows, half_rows, 0), 2)
        far = lax.ppermute(near, "dp", [(i, (i + 1) % n_groups) for i in range(n_groups)])
        w_out2 = jnp.where(group == 0, jnp.concatenate([near, far]), jnp.concatenate([far, near]))
        w_out_of = [w_out_flat, swap(w_out_flat, 1), w_out2, swap(w_out2, 1)]
        w_up_of = [w_up, swap(w_up, 1)]
        b_up_of = [row(b_up), swap(row(b_up), 1)]
        w_down_of = [w_down, swap(w_down, 1)]

        gain1, shift1, gain2, shift2 = row(ln1_gain), row(ln1_bias), row(ln2_gain), row(ln2_bias)
        me_array = jnp.reshape(me, (1,)).astype(jnp.int32)

        every_local = [piece for s in range(n_mine) for piece in x_local[s]]
        local = []
        for t in range(2):
            local += qkv_projection(every_local, gain1, shift1, w_qkv_of[t:t + 1], b_qkv_of[t:t + 1])
        ctx_own, ctx_far = [], []
        for s in range(n_mine):
            remote = qkv_projection(x_remote[s], gain1, shift1, w_qkv_of, b_qkv_of)
            own, far_ctx = [], []
            for t in range(2):
                own.append(attention(me_array, local[t], s, remote[t], n_heads, head_dim))
                far_ctx.append(swap(own[t], 2))
            ctx_own.append(own)
            ctx_far.append(far_ctx)

        def second_half(s, half, x, keep, out_type):
            resid, normed = out_projection(
                x, row(b_out), gain2, shift2, ctx_own[s] + ctx_far[s], [half, half, 1 - half, 1 - half], w_out_of, keep)
            return resid, mlp(normed, w_up_of, b_up_of, w_down_of, out_type)

        arrived = []
        for s in range(n_mine):
            _, part = second_half(s, 1, x_remote[s], False, BF16)
            arrived.append(swap(part, 2))
        core_array = jnp.reshape(core, (1,)).astype(jnp.int32)
        out, pieces = None, []
        for s in range(n_mine):
            resid, part = second_half(s, 0, x_local[s], True, F32)
            out, piece = finish(core_array, part, arrived[s], resid, row(b_down), s, n_batch, out)
            pieces.append(swap(piece, 1))
        for s in range(n_mine):
            out = place(core_array, pieces[s], s, out)
        return out

    in_layout = (P("dp", "tp", None), P(), P(), P(None, None, "tp", None), P(None, "tp", None), P("tp", None, None), P(), P(), P(), P(None, "tp"), P("tp"), P("tp", None), P())
    return jax.shard_map(device_body, mesh=mesh, in_specs=in_layout, out_specs=P("dp", "tp", None), check_vma=False)
```

```python
import functools
import math

import jax
import jax.numpy as jnp
from jax import lax
from jax.experimental import pallas as pl
from jax.experimental.pallas import tpu as pltpu
from jax.sharding import PartitionSpec as P


LN_EPS = 1e-5
BF16 = jnp.bfloat16
F32 = jnp.float32


CHUNK = 64
VMEM_MIB = 60
ANY = pl.BlockSpec(memory_space=pl.ANY)
WHOLE = pl.BlockSpec(memory_space=pltpu.VMEM)
SMEM = pl.BlockSpec(memory_space=pltpu.SMEM)


def normalize(x, gain, shift):
    as_f32 = x.astype(F32)
    row_mean = jnp.mean(as_f32, axis=-1, keepdims=True)
    centered = as_f32 - row_mean
    variance = jnp.mean(centered * centered, axis=-1, keepdims=True)
    return (centered * lax.rsqrt(variance + LN_EPS) * gain + shift).astype(BF16)


def params(**kwargs):
    return pltpu.CompilerParams(vmem_limit_bytes=VMEM_MIB << 20, **kwargs)


def cost(flops, moved, transcendentals=0):
    return pl.CostEstimate(flops=flops, bytes_accessed=moved, transcendentals=transcendentals)


def qkv_kernel(n_x, n_w, tile, *refs):
    x_refs, refs = refs[:n_x], refs[n_x:]
    gain_ref, shift_ref, bias_ref, refs = refs[0], refs[1], refs[2], refs[3:]
    w_refs, (out_ref, x_buf, normed, w_buf, x_sem, w_sem) = refs[:n_w], refs[n_w:]
    block = x_refs[0].shape[1]
    sub = tile // 2
    per_w = w_refs[0].shape[0] // sub
    steps = n_w * per_w // 2

    def fetch(n, go):
        slot = lax.rem(n, 2)
        for h in range(2):
            q = 2 * n + h
            if not go:
                pltpu.make_async_copy(w_refs[0].at[pl.ds(0, sub)], w_buf.at[slot, pl.ds(h * sub, sub)], w_sem.at[slot, h]).wait()
                continue
            for t in range(n_w):
                @pl.when((q >= t * per_w) & (q < (t + 1) * per_w))
                def _():
                    rows = pl.ds(pl.multiple_of((q - t * per_w) * sub, sub), sub)
                    pltpu.make_async_copy(w_refs[t].at[rows], w_buf.at[slot, pl.ds(h * sub, sub)], w_sem.at[slot, h]).start()

    copies = [pltpu.make_async_copy(x_refs[p].at[0], x_buf.at[pl.ds(p * block, block)], x_sem.at[p]) for p in range(n_x)]
    for c in copies:
        c.start()
    fetch(0, True)
    for p, c in enumerate(copies):
        c.wait()

        @pl.loop(0, block // CHUNK)
        def _(r):
            rows = pl.ds(pl.multiple_of(p * block + r * CHUNK, CHUNK), CHUNK)
            normed[rows, :] = normalize(x_buf[rows, :], gain_ref[...], shift_ref[...])

    @pl.loop(0, steps)
    def _(n):
        @pl.when(n + 1 < steps)
        def _():
            fetch(n + 1, True)

        fetch(n, False)
        acc = lax.dot_general(normed[...], w_buf[lax.rem(n, 2)], (((1,), (1,)), ((), ())), preferred_element_type=F32)
        cols = pl.ds(pl.multiple_of(n * tile, tile), tile)
        out = (acc + bias_ref[:, cols].astype(F32)).astype(BF16)
        out_ref[:, :, cols] = out.reshape(n_x, block, tile)


def qkv_projection(xs, gain, shift, bias, ws):
    n_x, n_w = len(xs), len(ws)
    _, block, d_model = xs[0].shape
    n_cols = n_w * ws[0].shape[0]
    tile = 768
    return pl.pallas_call(
        functools.partial(qkv_kernel, n_x, n_w, tile),
        out_shape=jax.ShapeDtypeStruct((n_x, block, n_cols), BF16),
        in_specs=[ANY] * n_x + [WHOLE] * 3 + [ANY] * n_w,
        out_specs=WHOLE,
        scratch_shapes=[
            pltpu.VMEM((n_x * block, d_model), BF16),
            pltpu.VMEM((n_x * block, d_model), BF16),
            pltpu.VMEM((2, tile, d_model), BF16),
            pltpu.SemaphoreType.DMA((n_x,)),
            pltpu.SemaphoreType.DMA((2, 2)),
        ],
        compiler_params=params(),
        cost_estimate=cost(2 * n_x * block * d_model * n_cols, 2 * (n_x * block * (d_model + n_cols) + n_cols * d_model)),
    )(*xs, gain, shift, bias, *ws)


def attention_kernel(n_heads, head_dim, window, me_ref, local_ref, remote_ref, near_ref, far_ref, ordered, ctx_ref):
    head = pl.program_id(1)
    me = me_ref[0]
    n_slots, block, width = ctx_ref.shape
    half = n_slots // 2

    @pl.when(head == 0)
    def _():
        for slot in range(n_slots):
            source = local_ref if slot < half else remote_ref
            ordered[me ^ slot] = source[slot % half]

    first = head * head_dim
    start = jnp.minimum((first // 128) * 128, width - window)
    start = pl.multiple_of(start, 128)
    lane = lax.broadcasted_iota(jnp.int32, (block, window), 1) + start
    in_head = (lane >= first) & (lane < first + head_dim)
    to_exp2 = head_dim ** -0.5 * math.log2(math.e)
    rows = lax.broadcasted_iota(jnp.int32, (block, block), 0)
    cols = lax.broadcasted_iota(jnp.int32, (block, block), 1)
    contract_last = (((1,), (1,)), ((), ()))
    for g in range(n_slots):
        q = ordered[g, :, pl.ds(start, window)]
        q = jnp.where(in_head, q, jnp.zeros_like(q))
        diag_k = ordered[g, :, pl.ds(width + start, window)]
        diag = lax.dot_general(q, diag_k, contract_last, preferred_element_type=F32)
        diag = jnp.where(rows >= cols, diag, -1e30)
        row_max = jnp.max(diag, axis=-1, keepdims=True)
        if g:
            k = ordered[0:g, :, pl.ds(width + start, window)].reshape(g * block, window)
            full = lax.dot_general(q, k, contract_last, preferred_element_type=F32)
            row_max = jnp.maximum(row_max, jnp.max(full, axis=-1, keepdims=True))
        diag = jnp.exp2((diag - row_max) * to_exp2)
        total = jnp.sum(diag, axis=-1, keepdims=True)
        if g:
            full = jnp.exp2((full - row_max) * to_exp2)
            total = total + jnp.sum(full, axis=-1, keepdims=True)
        inverse = 1.0 / total
        diag_v = ordered[g, :, pl.ds(2 * width + start, window)]
        ctx = jnp.dot((diag * inverse).astype(BF16), diag_v, preferred_element_type=F32)
        if g:
            v = ordered[0:g, :, pl.ds(2 * width + start, window)].reshape(g * block, window)
            ctx = ctx + jnp.dot((full * inverse).astype(BF16), v, preferred_element_type=F32)
        slot = me ^ g
        old = ctx_ref[slot, :, pl.ds(start, window)]
        ctx_ref[slot, :, pl.ds(start, window)] = jnp.where(in_head, ctx.astype(BF16), old)

    @pl.when(head == n_heads - 1)
    def _():
        near_ref[...] = ctx_ref[0:half]
        far_ref[...] = ctx_ref[half:]


def attention(me, qkv_local, local_at, qkv_remote, n_groups, n_heads, head_dim):
    n_half, block, columns = qkv_remote.shape
    three_width = columns // n_groups
    width = three_width // 3
    n_slots = 2 * n_half
    window = 256
    pairs = n_groups * n_heads * n_slots * (n_slots + 1) // 2
    out = jax.ShapeDtypeStruct((n_half, block, n_groups * width), BF16)
    return pl.pallas_call(
        functools.partial(attention_kernel, n_heads, head_dim, window),
        out_shape=[out, out],
        grid_spec=pltpu.PrefetchScalarGridSpec(
            num_scalar_prefetch=1,
            grid=(n_groups, n_heads),
            in_specs=[
                pl.BlockSpec((n_half, block, three_width), lambda t, j, me: (local_at, 0, t)),
                pl.BlockSpec((n_half, block, three_width), lambda t, j, me: (0, 0, t)),
            ],
            out_specs=[pl.BlockSpec((n_half, block, width), lambda t, j, me: (0, 0, t))] * 2,
            scratch_shapes=[pltpu.VMEM((n_slots, block, three_width), BF16), pltpu.VMEM((n_slots, block, width), BF16)],
        ),
        compiler_params=params(dimension_semantics=("arbitrary", "arbitrary")),
        cost_estimate=cost(pairs * block * block * window * 4, n_groups * n_slots * block * width * 8, pairs * block * block),
    )(me, qkv_local, qkv_remote)


def tail_kernel(keep, n_w, out_tile, tile, x0, x1, c_near, c_far, *refs):
    wout_refs, refs = refs[:2 * n_w], refs[2 * n_w:]
    up_refs, down_refs, refs = refs[:n_w], refs[n_w:2 * n_w], refs[2 * n_w:]
    (bout_ref, gain_ref, shift_ref, bup_ref, bdown_ref, out0, out1,
     x_buf, ctx, normed, wout_buf, up_buf, down_buf, acc, x_sem, c_sem, wout_sem, up_sem, down_sem) = refs
    rows_all, d_model = x_buf.shape
    block = rows_all // 2
    width = wout_refs[0].shape[0]
    out_steps = d_model // out_tile
    per_w = up_refs[0].shape[1] // tile
    steps = n_w * per_w

    def fetch_out(n, go):
        slot = lax.rem(n, 2)
        cols = pl.ds(pl.multiple_of(n * out_tile, out_tile), out_tile)
        for j, w in enumerate(wout_refs):
            copy = pltpu.make_async_copy(w.at[:, cols], wout_buf.at[slot, pl.ds(j * width, width)], wout_sem.at[slot, j])
            copy.start() if go else copy.wait()

    def fetch_mlp(n, go):
        slot = lax.rem(n, 2)
        for t in range(n_w if go else 1):
            def transfer(at):
                part = pl.ds(pl.multiple_of(at * tile, tile), tile)
                up = pltpu.make_async_copy(up_refs[t].at[:, part], up_buf.at[slot], up_sem.at[slot])
                down = pltpu.make_async_copy(down_refs[t].at[part, :], down_buf.at[slot], down_sem.at[slot])
                return up, down

            if go:
                @pl.when((n >= t * per_w) & (n < (t + 1) * per_w))
                def _():
                    for copy in transfer(n - t * per_w):
                        copy.start()
            else:
                for copy in transfer(0):
                    copy.wait()

    copies = []
    for j, c in enumerate((c_near, c_far)):
        for p in range(2):
            copies.append(pltpu.make_async_copy(
                c.at[p], ctx.at[pl.ds(p * block, block), pl.ds(j * n_w * width, n_w * width)], c_sem.at[j, p]))
    for c in copies:
        c.start()
    fetch_out(0, True)
    for p, x in enumerate((x0, x1)):
        copies.append(pltpu.make_async_copy(x.at[0], x_buf.at[pl.ds(p * block, block)], x_sem.at[p]))
        copies[-1].start()
    fetch_mlp(0, True)
    for c in copies:
        c.wait()

    @pl.loop(0, out_steps)
    def _(n):
        @pl.when(n + 1 < out_steps)
        def _():
            fetch_out(n + 1, True)

        fetch_out(n, False)
        cols = pl.ds(pl.multiple_of(n * out_tile, out_tile), out_tile)
        part = jnp.dot(ctx[...], wout_buf[lax.rem(n, 2)], preferred_element_type=F32) + bout_ref[:, cols].astype(F32)
        x_buf[:, cols] = (x_buf[:, cols].astype(F32) + part).astype(BF16)

    @pl.loop(0, rows_all // CHUNK)
    def _(r):
        rows = pl.ds(pl.multiple_of(r * CHUNK, CHUNK), CHUNK)
        resid = x_buf[rows, :]
        normed[rows, :] = normalize(resid, gain_ref[...], shift_ref[...])
        if keep:
            acc[rows, :] = resid.astype(F32) + bdown_ref[...].astype(F32)
        else:
            acc[rows, :] = jnp.zeros_like(acc[rows, :])

    @pl.loop(0, steps)
    def _(n):
        @pl.when(n + 1 < steps)
        def _():
            fetch_mlp(n + 1, True)

        fetch_mlp(n, False)
        slot = lax.rem(n, 2)
        up = jnp.dot(normed[...], up_buf[slot], preferred_element_type=F32) + bup_ref[n].astype(F32)
        act = jax.nn.gelu(up, approximate=True).astype(BF16)
        acc[...] += jnp.dot(act, down_buf[slot], preferred_element_type=F32)

    out0[...] = acc[0:block].astype(out0.dtype)
    out1[...] = acc[block:].astype(out1.dtype)


def tail(xs, c_near, c_far, w_outs, ups, downs, vectors, b_up, b_down, keep):
    _, block, d_model = xs[0].shape
    width = w_outs[0].shape[0]
    n_w = len(ups)
    n_cols = ups[0].shape[1]
    out_tile = tile = 512
    rows = 2 * block
    out = jax.ShapeDtypeStruct((block, d_model), F32 if keep else BF16)
    total = n_w * n_cols
    return pl.pallas_call(
        functools.partial(tail_kernel, keep, n_w, out_tile, tile),
        out_shape=[out, out],
        in_specs=[ANY] * (4 + 4 * n_w) + [WHOLE] * 5,
        out_specs=[WHOLE, WHOLE],
        scratch_shapes=[
            pltpu.VMEM((rows, d_model), BF16),
            pltpu.VMEM((rows, 2 * n_w * width), BF16),
            pltpu.VMEM((rows, d_model), BF16),
            pltpu.VMEM((2, 2 * n_w * width, out_tile), BF16),
            pltpu.VMEM((2, d_model, tile), BF16),
            pltpu.VMEM((2, tile, d_model), BF16),
            pltpu.VMEM((rows, d_model), F32),
            pltpu.SemaphoreType.DMA((2,)),
            pltpu.SemaphoreType.DMA((2, 2)),
            pltpu.SemaphoreType.DMA((2, 2 * n_w)),
            pltpu.SemaphoreType.DMA((2,)),
            pltpu.SemaphoreType.DMA((2,)),
        ],
        compiler_params=params(),
        cost_estimate=cost(
            2 * rows * d_model * (2 * n_w * width + 2 * total),
            2 * (rows * 4 * d_model + 2 * n_w * width * d_model + 2 * total * d_model),
            rows * total),
    )(*xs, c_near, c_far, *w_outs, *ups, *downs, *vectors, b_up.reshape(total // tile, 1, tile), b_down)


def finish_kernel(core_ref, base_ref, arrived_ref, *refs):
    out_ref = refs[-1]
    out_ref[...] = (base_ref[...] + arrived_ref[...].astype(F32)).astype(BF16).reshape(out_ref.shape)


def place_kernel(core_ref, block_ref, out_in_ref, out_ref):
    out_ref[0] = block_ref[...]


def finish(core, base, arrived, s, n_batch, out):
    block, d_model = base.shape
    n_mine = n_batch // 2
    tile = 128
    spec = pl.BlockSpec((tile, d_model), lambda i, c: (i, 0))
    extra = [] if out is None else [out]
    return pl.pallas_call(
        finish_kernel,
        out_shape=jax.ShapeDtypeStruct((n_batch, block, d_model), BF16),
        grid_spec=pltpu.PrefetchScalarGridSpec(
            num_scalar_prefetch=1,
            grid=(block // tile,),
            in_specs=[spec, spec] + [ANY] * len(extra),
            out_specs=pl.BlockSpec((1, tile, d_model), lambda i, c: (c[0] * n_mine + s, i, 0)),
        ),
        input_output_aliases={3: 0} if extra else {},
        compiler_params=params(),
        cost_estimate=cost(block * d_model * 2, 8 * block * d_model),
    )(core, base, arrived, *extra)


def finish_other(core, base, arrived):
    block, d_model = base.shape
    tile = 128
    spec = pl.BlockSpec((tile, d_model), lambda i, c: (i, 0))
    return pl.pallas_call(
        finish_kernel,
        out_shape=jax.ShapeDtypeStruct((block, d_model), BF16),
        grid_spec=pltpu.PrefetchScalarGridSpec(num_scalar_prefetch=1, grid=(block // tile,), in_specs=[spec, spec], out_specs=spec),
        compiler_params=params(),
        cost_estimate=cost(block * d_model * 2, 8 * block * d_model),
    )(core, base, arrived)


def place(core, piece, s, out):
    n_batch, block, d_model = out.shape
    n_mine = n_batch // 2
    tile = 128
    return pl.pallas_call(
        place_kernel,
        out_shape=jax.ShapeDtypeStruct(out.shape, BF16),
        grid_spec=pltpu.PrefetchScalarGridSpec(
            num_scalar_prefetch=1,
            grid=(block // tile,),
            in_specs=[pl.BlockSpec((tile, d_model), lambda i, c: (i, 0)), ANY],
            out_specs=pl.BlockSpec((1, tile, d_model), lambda i, c: ((1 - c[0]) * n_mine + s, i, 0)),
        ),
        input_output_aliases={2: 0},
        compiler_params=params(),
        cost_estimate=cost(block * d_model, 4 * block * d_model),
    )(core, piece, out)


def solution(mesh):
    group_size = mesh.shape["tp"]
    n_groups = mesh.shape["dp"]

    def swap(array, mask):
        return lax.ppermute(array, "tp", [(i, i ^ mask) for i in range(group_size)])

    def device_body(hidden, ln1_gain, ln1_bias, w_qkv, b_qkv, w_out, b_out, ln2_gain, ln2_bias, w_up, b_up, w_down, b_down):
        n_batch, _, d_model = hidden.shape
        _, _, n_heads, head_dim = w_qkv.shape
        width = n_heads * head_dim
        me = lax.axis_index("tp")
        core = me % 2
        group = lax.axis_index("dp")
        n_mine = n_batch // 2
        row = lambda v: v.reshape(1, -1)
        me_array = jnp.reshape(me, (1,)).astype(jnp.int32)
        core_array = jnp.reshape(core, (1,)).astype(jnp.int32)

        slots = [[None] * group_size for _ in range(n_mine)]
        others = []
        source = hidden
        for s in range(n_mine):
            slots[s][0] = lax.dynamic_slice_in_dim(source, core * n_mine + s, 1, 0)
            slots[s][2] = swap(slots[s][0], 2)
            source, _ = lax.optimization_barrier((source, slots[s][0]))
            others.append(lax.dynamic_slice_in_dim(source, (1 - core) * n_mine + s, 1, 0))
            slots[s][3] = swap(others[s], 3)
            slots[s][1] = swap(others[s], 1)
            source, _ = lax.optimization_barrier((source, others[s]))

        biases = jnp.concatenate([b_qkv.reshape(-1), b_up])
        biases_of = [biases, swap(biases, 1)]
        b_qkv_all = row(jnp.concatenate([b[:3 * width] for b in biases_of]))
        b_up_all = jnp.concatenate([b[3 * width:] for b in biases_of])
        w_qkv_t = jnp.transpose(w_qkv, (1, 2, 3, 0)).reshape(3 * width, d_model)
        w_qkv_of = [w_qkv_t, swap(w_qkv_t, 1)]
        w_out_flat = w_out.reshape(width, d_model)
        half_rows = width // n_groups
        near = swap(lax.dynamic_slice_in_dim(w_out_flat, group * half_rows, half_rows, 0), 2)
        far = lax.ppermute(near, "dp", [(i, (i + 1) % n_groups) for i in range(n_groups)])
        w_out2 = jnp.where(group == 0, jnp.concatenate([near, far]), jnp.concatenate([far, near]))
        w_out_of = [w_out_flat, swap(w_out_flat, 1), w_out2, swap(w_out2, 1)]
        w_up_of = [w_up, swap(w_up, 1)]
        w_down_of = [w_down, swap(w_down, 1)]

        gain1, shift1 = row(ln1_gain), row(ln1_bias)
        local = qkv_projection([x for s in range(n_mine) for x in slots[s][:2]], gain1, shift1, b_qkv_all, w_qkv_of)
        near_ctx, far_ctx, arrived_near, arrived_far = [], [], [], []
        for s in range(n_mine):
            remote = qkv_projection(slots[s][2:], gain1, shift1, b_qkv_all, w_qkv_of)
            a, b = attention(me_array, local, s, remote, 2, n_heads, head_dim)
            near_ctx.append(a)
            far_ctx.append(b)
            arrived_near.append(swap(a, 2))
            arrived_far.append(swap(b, 2))

        vectors = (row(b_out), row(ln2_gain), row(ln2_bias))
        from_other = []
        for s in range(n_mine):
            part2, part3 = tail(slots[s][2:], far_ctx[s], arrived_near[s], w_out_of, w_up_of, w_down_of, vectors, b_up_all, row(b_down), False)
            from_other.append((swap(part3, 2), swap(part2, 2)))
        bases = []
        for s in range(n_mine):
            bases.append(tail(slots[s][:2], near_ctx[s], arrived_far[s], w_out_of, w_up_of, w_down_of, vectors, b_up_all, row(b_down), True))
        out, pieces = None, []
        for s in range(n_mine):
            piece = finish_other(core_array, bases[s][1], from_other[s][0])
            pieces.append(swap(piece, 1))
            if s == n_mine - 1:
                for k in range(n_mine):
                    out = place(core_array, pieces[k], k, out)
            out = finish(core_array, bases[s][0], from_other[s][1], s, n_batch, out)
        return out

    in_layout = (P("dp", "tp", None), P(), P(), P(None, None, "tp", None), P(None, "tp", None), P("tp", None, None), P(), P(), P(), P(None, "tp"), P("tp"), P("tp", None), P())
    return jax.shard_map(device_body, mesh=mesh, in_specs=in_layout, out_specs=P("dp", "tp", None), check_vma=False)
```
